256 devices in a mesh: replica: 16 (over z_lo, y, core), model: 16 (over z_hi, x).
Axes of the slice: x: 4, y: 4, z: 8 (z_hi: 4, z_lo: 2; z = z_hi * 2 + z_lo), core: 2. Of those that a mesh axis runs over, the one named last changes fastest.
Arguments:
- partial_query: float32 [16, 2048, 2048], P('replica', None, 'model'), may hold values from -4 to 4
- partial_key: float32 [16, 2048, 2048], P('replica', None, 'model'), may hold values from -4 to 4
- partial_value: float32 [16, 2048, 2048], P('replica', None, 'model'), may hold values from -4 to 4
- partial_mixed: float32 [16, 2048, 2048], P('replica', 'model'), may hold values from -4 to 4
- partial_norm: float32 [16, 2048], P('replica'), may hold values from -8 to 8
- partial_bias: float32 [16, 2048], P('replica'), may hold values from -8 to 8
- master_query: float32 [2048, 2048], P('replica', 'model'), may hold values from -0.1875 to 0.1875
- master_key: float32 [2048, 2048], P('replica', 'model'), may hold values from -0.1875 to 0.1875
- master_value: float32 [2048, 2048], P('replica', 'model'), may hold values from -0.1875 to 0.1875
- master_mixed: float32 [2048, 2048], P('model', 'replica'), may hold values from -0.1875 to 0.1875
- master_norm: float32 [2048], P('replica'), may hold values from 0.25 to 1.75
- master_bias: float32 [2048], P('replica'), may hold values from -3 to 3
- memory_query: float32 [2048, 2048], P('replica', 'model'), may hold values from 9.765625e-05 to 0.0009765625
- memory_key: float32 [2048, 2048], P('replica', 'model'), may hold values from 9.765625e-05 to 0.0009765625
- memory_value: float32 [2048, 2048], P('replica', 'model'), may hold values from 9.765625e-05 to 0.0009765625
- memory_mixed: float32 [2048, 2048], P('model', 'replica'), may hold values from 9.765625e-05 to 0.0009765625
- memory_norm: float32 [2048], P('replica'), may hold values from 0.05 to 0.8
- memory_bias: float32 [2048], P('replica'), may hold values from 0.05 to 0.8
Outputs:
- compute_query: bfloat16 [2048, 2048], P(None, 'model')
- compute_key: bfloat16 [2048, 2048], P(None, 'model')
- compute_value: bfloat16 [2048, 2048], P(None, 'model')
- compute_mixed: bfloat16 [2048, 2048], P('model')
- compute_norm: bfloat16 [2048], replicated
- compute_bias: bfloat16 [2048], replicated
- stepped_query: float32 [2048, 2048], P('replica', 'model')
- stepped_key: float32 [2048, 2048], P('replica', 'model')
- stepped_value: float32 [2048, 2048], P('replica', 'model')
- stepped_mixed: float32 [2048, 2048], P('model', 'replica')
- stepped_norm: float32 [2048], P('replica')
- stepped_bias: float32 [2048], P('replica')
- state_new_query: float32 [2048, 2048], P('replica', 'model')
- state_new_key: float32 [2048, 2048], P('replica', 'model')
- state_new_value: float32 [2048, 2048], P('replica', 'model')
- state_new_mixed: float32 [2048, 2048], P('model', 'replica')
- state_new_norm: float32 [2048], P('replica')
- state_new_bias: float32 [2048], P('replica')
The draws below stay inside these ranges and needn't reach their ends.
All inputs are finite; a program needn't handle non-finite values.
Results may differ from the reference program's by a relative error of at most 0.0004.
Values may be sent and summed in bfloat16 or wider, within the bound.
A program may use at most 64 MiB of HBM per device.

```python
import jax
import jax.numpy as jnp
from jax import lax

WIDTH = 2048
ATTN = 2048
REPLICAS = 16


def with_spikes(drawn, stream_key, source, target, shards_of, factor):
    def block_of(axis_at):
        return (jnp.arange(drawn.shape[axis_at]) // (drawn.shape[axis_at] // shards_of)).reshape((-1,) + (1,) * (drawn.ndim - 1 - axis_at))

    first = jax.random.permutation(stream_key, shards_of)[block_of(target)]
    second = (block_of(target) + shards_of // 2) % shards_of
    return jnp.where((block_of(source) == first) | (block_of(source) == second), factor * drawn, drawn)


def block_scale(key, extent, split, smallest, high):
    gain, own = 1.0, jax.random.fold_in(key, 6)
    for dim, parts in split:
        draws = jnp.exp(jax.random.uniform(jax.random.fold_in(own, dim), (parts,), jnp.float32, smallest / len(split), high / len(split)))
        gain = gain * jnp.repeat(draws, extent[dim] // parts).reshape([-1 if axis == dim else 1 for axis in range(len(extent))])
    return gain


def noise(rng, shape, scale, reach, split=(), dtype=jnp.bfloat16):
    values = jax.random.normal(rng, shape, jnp.float32) * scale
    if len(split) > 0:
        values = block_scale(rng, shape, split, -0.22, 0.18) * values
    return jnp.clip(values, min=-reach, max=reach).astype(dtype)


def gaussian_with(own_key, dims, width, bound, pieces, heavy, held_as=jnp.bfloat16):
    array = width * jax.random.normal(own_key, dims, jnp.float32)
    if pieces:
        array = array * block_scale(own_key, dims, pieces, -0.22, 0.18)
    return jnp.clip(with_spikes(array, jax.random.fold_in(own_key, 3), *heavy), -bound, bound).astype(held_as)


def setup_inputs(seed: int = 0) -> dict:
    keys = jax.random.split(jax.random.key(seed), 19)
    return {
        "partial_query": gaussian_with(keys[0], (REPLICAS, WIDTH, ATTN), 0.5, 4.0, ((0, 16), (2, 16)), (0, 1, 16, 2.0), jnp.float32),
        "partial_key": gaussian_with(keys[1], (REPLICAS, WIDTH, ATTN), 0.5, 4.0, ((0, 16), (2, 16)), (0, 1, 16, 2.0), jnp.float32),
        "partial_value": gaussian_with(keys[2], (REPLICAS, WIDTH, ATTN), 0.5, 4.0, ((0, 16), (2, 16)), (0, 1, 16, 2.0), jnp.float32),
        "partial_mixed": gaussian_with(keys[3], (REPLICAS, ATTN, WIDTH), 0.5, 4.0, ((0, 16), (1, 16)), (0, 2, 16, 2.0), jnp.float32),
        "partial_norm": gaussian_with(keys[4], (REPLICAS, WIDTH), 1.0, 8.0, ((0, 16),), (0, 1, 16, 2.0), jnp.float32),
        "partial_bias": gaussian_with(keys[5], (REPLICAS, WIDTH), 1.0, 8.0, ((0, 16),), (0, 1, 16, 2.0), jnp.float32),
        "master_query": gaussian_with(keys[6], (WIDTH, ATTN), WIDTH ** -0.5, 0.1875, ((0, 16), (1, 16)), (1, 0, 16, 2.0), jnp.float32),
        "master_key": gaussian_with(keys[7], (WIDTH, ATTN), WIDTH ** -0.5, 0.1875, ((0, 16), (1, 16)), (1, 0, 16, 2.0), jnp.float32),
        "master_value": gaussian_with(keys[8], (WIDTH, ATTN), WIDTH ** -0.5, 0.1875, ((0, 16), (1, 16)), (1, 0, 16, 2.0), jnp.float32),
        "master_mixed": gaussian_with(keys[9], (ATTN, WIDTH), ATTN ** -0.5, 0.1875, ((0, 16), (1, 16)), (0, 1, 16, 2.0), jnp.float32),
        "master_norm": jnp.clip(1.0 + 0.15 * jax.random.normal(keys[10], (WIDTH,), jnp.float32), 0.25, 1.75),
        "master_bias": noise(keys[11], (WIDTH,), 0.5, 3.0, ((0, 16),), jnp.float32),
        "memory_query": jnp.clip(9.765625145519152e-05 + 0.0008789062 * jax.random.uniform(keys[12], (WIDTH, ATTN), jnp.float32) ** block_scale(keys[12], (WIDTH, ATTN), ((0, 16), (1, 16)), -0.2, 0.2), 9.765625145519152e-05, 0.0009765625),
        "memory_key": jnp.clip(9.765625145519152e-05 + 0.0008789062 * jax.random.uniform(keys[13], (WIDTH, ATTN), jnp.float32) ** block_scale(keys[13], (WIDTH, ATTN), ((0, 16), (1, 16)), -0.2, 0.2), 9.765625145519152e-05, 0.0009765625),
        "memory_value": jnp.clip(9.765625145519152e-05 + 0.0008789062 * jax.random.uniform(keys[14], (WIDTH, ATTN), jnp.float32) ** block_scale(keys[14], (WIDTH, ATTN), ((0, 16), (1, 16)), -0.2, 0.2), 9.765625145519152e-05, 0.0009765625),
        "memory_mixed": jnp.clip(9.765625145519152e-05 + 0.0008789062 * jax.random.uniform(keys[15], (ATTN, WIDTH), jnp.float32) ** block_scale(keys[15], (ATTN, WIDTH), ((0, 16), (1, 16)), -0.2, 0.2), 9.765625145519152e-05, 0.0009765625),
        "memory_norm": jnp.clip(0.05 + 0.75 * jax.random.uniform(keys[16], (WIDTH,), jnp.float32) ** block_scale(keys[16], (WIDTH,), ((0, 16),), -0.2, 0.2), 0.05, 0.8),
        "memory_bias": jnp.clip(0.05 + 0.75 * jax.random.uniform(keys[17], (WIDTH,), jnp.float32) ** block_scale(keys[17], (WIDTH,), ((0, 16),), -0.2, 0.2), 0.05, 0.8),
    }


learn_rate = 0.015
hold_rate = 0.8

def reference(partial_query, partial_key, partial_value, partial_mixed, partial_norm, partial_bias, master_query, master_key, master_value, master_mixed, master_norm, master_bias, memory_query, memory_key, memory_value, memory_mixed, memory_norm, memory_bias):
    mean_query = lax.optimization_barrier(jnp.sum(partial_query.astype(jnp.float32), axis=0)) * REPLICAS ** (-0.5)
    mean_key = lax.optimization_barrier(jnp.sum(partial_key.astype(jnp.float32), axis=0)) * REPLICAS ** (-0.5)
    mean_value = lax.optimization_barrier(jnp.sum(partial_value.astype(jnp.float32), axis=0)) * REPLICAS ** (-0.5)
    mean_mixed = lax.optimization_barrier(jnp.sum(partial_mixed.astype(jnp.float32), axis=0)) * REPLICAS ** (-0.5)
    mean_norm = lax.optimization_barrier(jnp.sum(partial_norm.astype(jnp.float32), axis=0)) * REPLICAS ** (-0.5)
    mean_bias = lax.optimization_barrier(jnp.sum(partial_bias.astype(jnp.float32), axis=0)) * REPLICAS ** (-0.5)
    ratio_query = jnp.sqrt(lax.optimization_barrier(jnp.sum(master_query * master_query, axis=1, keepdims=True))) * lax.rsqrt(lax.optimization_barrier(jnp.sum(mean_query * mean_query, axis=1, keepdims=True)) + 1e-06)
    mean_query = mean_query * ratio_query
    ratio_key = jnp.sqrt(lax.optimization_barrier(jnp.sum(master_key * master_key, axis=1, keepdims=True))) * lax.rsqrt(lax.optimization_barrier(jnp.sum(mean_key * mean_key, axis=1, keepdims=True)) + 1e-06)
    mean_key = mean_key * ratio_key
    ratio_value = jnp.sqrt(lax.optimization_barrier(jnp.sum(master_value * master_value, axis=1, keepdims=True))) * lax.rsqrt(lax.optimization_barrier(jnp.sum(mean_value * mean_value, axis=1, keepdims=True)) + 1e-06)
    mean_value = mean_value * ratio_value
    ratio_mixed = jnp.sqrt(lax.optimization_barrier(jnp.sum(master_mixed * master_mixed, axis=0, keepdims=True))) * lax.rsqrt(lax.optimization_barrier(jnp.sum(mean_mixed * mean_mixed, axis=0, keepdims=True)) + 1e-06)
    mean_mixed = mean_mixed * ratio_mixed
    state_new_query = hold_rate * memory_query + (1.0 - hold_rate) * mean_query * mean_query
    stepped_query = master_query - learn_rate * mean_query * lax.rsqrt(state_new_query + 1e-06)
    state_new_key = hold_rate * memory_key + (1.0 - hold_rate) * mean_key * mean_key
    stepped_key = master_key - learn_rate * mean_key * lax.rsqrt(state_new_key + 1e-06)
    state_new_value = hold_rate * memory_value + (1.0 - hold_rate) * mean_value * mean_value
    stepped_value = master_value - learn_rate * mean_value * lax.rsqrt(state_new_value + 1e-06)
    state_new_mixed = hold_rate * memory_mixed + (1.0 - hold_rate) * mean_mixed * mean_mixed
    stepped_mixed = master_mixed - learn_rate * mean_mixed * lax.rsqrt(state_new_mixed + 1e-06)
    state_new_norm = hold_rate * memory_norm + (1.0 - hold_rate) * mean_norm * mean_norm
    stepped_norm = master_norm - learn_rate * mean_norm * lax.rsqrt(state_new_norm + 1e-06)
    state_new_bias = hold_rate * memory_bias + (1.0 - hold_rate) * mean_bias * mean_bias
    stepped_bias = master_bias - learn_rate * mean_bias * lax.rsqrt(state_new_bias + 1e-06)
    compute_query = stepped_query.astype(jnp.bfloat16)
    compute_key = stepped_key.astype(jnp.bfloat16)
    compute_value = stepped_value.astype(jnp.bfloat16)
    compute_mixed = stepped_mixed.astype(jnp.bfloat16)
    compute_norm = stepped_norm.astype(jnp.bfloat16)
    compute_bias = stepped_bias.astype(jnp.bfloat16)
    return (compute_query, compute_key, compute_value, compute_mixed, compute_norm, compute_bias, stepped_query, stepped_key, stepped_value, stepped_mixed, stepped_norm, stepped_bias, state_new_query, state_new_key, state_new_value, state_new_mixed, state_new_norm, state_new_bias)
```

```python
import functools

import jax
import jax.numpy as jnp
from jax import lax
from jax.experimental import pallas as pl
from jax.experimental.pallas import tpu as pltpu
from jax.sharding import PartitionSpec as P

LEARN_RATE = 0.015
HOLD_RATE = 0.8
F32, BF16 = jnp.float32, jnp.bfloat16

CODE_ROWS = 136


def turned(line, to_lanes):
    shape = (128, 128)
    same = lax.broadcasted_iota(jnp.int32, shape, 0) == lax.broadcasted_iota(jnp.int32, shape, 1)
    return jnp.sum(jnp.where(same, line, 0.0), axis=0 if to_lanes else 1, keepdims=True)


def encode(x, i):
    size = jnp.abs(x)
    top = jnp.max(size, axis=0 if i == 3 else 1, keepdims=True)
    top = (top * 1.004 + 1e-30).astype(BF16).astype(F32)
    size = size * (1.0 / top)
    code = jnp.exp2(250.0 * (size * lax.rsqrt(size + 1e-35)) - 125.0)
    code = jnp.where(x < 0, -code, code).astype(BF16)
    line = top if i == 3 else turned(top, True)
    return code, jnp.broadcast_to(line, (CODE_ROWS - 128, 128)).astype(BF16)


def decode(code, line, i):
    code = code.astype(F32)
    line = line.astype(F32)[0:1]
    top = line if i == 3 else turned(line, False)
    root = jnp.log2(jnp.abs(code)) * (1.0 / 250.0) + 0.5
    size = root * root * top
    return jnp.where(code < 0, -size, size)


def update(mean, master, memory):
    state = HOLD_RATE * memory + (1.0 - HOLD_RATE) * mean * mean
    return state, master - LEARN_RATE * mean * lax.rsqrt(state + 1e-06)


def kernel(*refs):
    (pq, pk, pv, pm, pn, pb, *rest) = refs
    masters, small_masters, memories, small_memories, rest = (
        rest[0:4], rest[4:6], rest[6:10], rest[10:12], rest[12:],
    )
    (
        g, stp, sta, sm_g, sm_stp, sm_sta,
        own, pair, snd, rcv, mean, mast, memo,
        sm_own, sm_pair, sm_snd, sm_rcv, sm_mast, sm_memo,
        psnd, prcv,
        own_sem, pair_s, pair_r, rs_s, rs_r, ps_s, ps_r, ag_s, ag_r, rl_s, rl_r,
        in_sem, smo_sem, smp_s, smp_r, smr_s, smr_r,
    ) = rest
    r, m = lax.axis_index("replica"), lax.axis_index("model")
    c = lax.rem(r, 2)
    chip = r // 2
    z, y = chip // 4, lax.rem(chip, 4)
    partner = r + 1 - 2 * c

    def to_chip(k):
        return lax.rem(z + k // 4, 2) * 4 + lax.rem(y + lax.rem(k, 4), 4)

    def from_chip(k):
        return lax.rem(z + k // 4, 2) * 4 + lax.rem(y + 4 - lax.rem(k, 4), 4)

    def remote(src, dst, send, recv, replica, model=None):
        return pltpu.make_async_remote_copy(
            src_ref=src, dst_ref=dst, send_sem=send, recv_sem=recv,
            device_id={"replica": replica, "model": m if model is None else model},
            device_id_type=pl.DeviceIdType.MESH,
        )

    barrier = pltpu.get_barrier_semaphore()

    def hail(replica, model):
        pl.semaphore_signal(
            barrier, inc=1, device_id={"replica": replica, "model": model},
            device_id_type=pl.DeviceIdType.MESH,
        )

    @pl.loop(1, 16)
    def _(j):
        hail(r, lax.rem(m + j, 16))

    @pl.loop(1, 8)
    def _(k):
        hail(2 * to_chip(k) + c, m)

    hail(partner, m)

    def cut(i, d, core):
        if i < 3:
            return (pq, pk, pv)[i].at[d, core]
        return pm.at[:, pl.ds(pl.multiple_of((2 * d + core) * 128, 128), 128)]

    def own_copy(i, d):
        return pltpu.make_async_copy(cut(i, d, c), own.at[i, d], own_sem.at[i, d])

    for i in range(4):
        @pl.loop(0, 8)
        def _(k):
            own_copy(i, to_chip(k)).start()

    small_in = [pltpu.make_async_copy(s, sm_own.at[i], smo_sem.at[i]) for i, s in enumerate((pn, pb))]
    loads = [
        pltpu.make_async_copy(s, d, in_sem.at[n])
        for n, (s, d) in enumerate(
            [(masters[i], mast.at[i]) for i in range(4)]
            + [(memories[i], memo.at[i]) for i in range(4)]
            + [(small_masters[i], sm_mast.at[i]) for i in range(2)]
            + [(small_memories[i], sm_memo.at[i]) for i in range(2)]
        )
    ]
    for copy in small_in + loads:
        copy.start()

    pl.semaphore_wait(barrier, 23)

    def pair_copy(i, d):
        return remote(cut(i, d, 1 - c), pair.at[i, d], pair_s.at[i, d], pair_r.at[i, d], partner)

    small_pair = [remote(s, sm_pair.at[i], smp_s.at[i], smp_r.at[i], partner) for i, s in enumerate((pn, pb))]
    for i in range(4):
        @pl.loop(1, 9)
        def _(k):
            pair_copy(i, to_chip(lax.rem(k, 8))).start()
        if i == 0:
            for copy in small_pair:
                copy.start()

    for copy in loads:
        copy.wait()

    def sizes(x, i):
        x = x * x
        return jnp.sum(x if i == 3 else jnp.transpose(x), axis=0, keepdims=True)

    for i in range(4):
        psnd[i, 1:2, :] = sizes(mast[i], i)

    def rs_copy(i, k):
        return remote(snd.at[i, k - 1], rcv.at[i, k - 1], rs_s.at[i, k - 1], rs_r.at[i, k - 1], 2 * to_chip(k) + c)

    for i in range(4):
        @pl.loop(1, 8)
        def _(k):
            d = to_chip(k)
            own_copy(i, d).wait()
            pair_copy(i, d).wait_recv()
            code, line = encode(own[i, d] + pair[i, d], i)
            snd[i, k - 1, 0:128] = code
            snd[i, k - 1, 128:CODE_ROWS] = line
            rs_copy(i, k).start()

        own_copy(i, chip).wait()
        pair_copy(i, chip).wait_recv()
        mean[i] = own[i, chip] + pair[i, chip]

        if i == 0:
            def small_copy(k):
                return remote(sm_snd.at[2 * to_chip(k) + c], sm_rcv.at[k - 1], smr_s.at[k - 1], smr_r.at[k - 1], 2 * to_chip(k) + c)

            for n in range(2):
                small_in[n].wait()
                small_pair[n].wait_recv()
                line = sm_own[n] + sm_pair[n]
                for b in range(16):
                    sm_snd[b, n : n + 1, :] = line[:, 128 * b : 128 * b + 128]

            @pl.loop(1, 8)
            def _(k):
                small_copy(k).start()

    def psum_copy(i, j):
        return remote(psnd.at[i], prcv.at[i, j - 1], ps_s.at[i, j - 1], ps_r.at[i, j - 1], r, lax.rem(m + j, 16))

    def add_up(i):
        def one(k, total):
            rs_copy(i, k).wait_recv()
            return total + decode(rcv[i, k - 1, 0:128], rcv[i, k - 1, 128:CODE_ROWS], i)

        total = lax.fori_loop(1, 8, one, mean[i]) * 0.25
        mean[i] = total
        psnd[i, 0:1, :] = sizes(total, i)

        @pl.loop(1, 16)
        def _(j):
            psum_copy(i, j).start()

    height = (144, 128, 128, 128)

    def ag_copy(i, k):
        b = g.at[i, r, 0 : height[i]]
        return remote(b, b, ag_s.at[i, k - 1], ag_r.at[i, k - 1], 2 * to_chip(k) + c)

    def relay_copy(i, d):
        b = g.at[i, 2 * d + c, 0 : height[i]]
        return remote(b, b, rl_s.at[i, d], rl_r.at[i, d], partner)

    def step(i):
        def one(j, total):
            psum_copy(i, j).wait_recv()
            return total + prcv[i, j - 1]

        total = lax.fori_loop(1, 16, one, psnd[i])
        ratio = jnp.sqrt(total[1:2]) * lax.rsqrt(total[0:1] + 1e-06)
        ratio = jnp.broadcast_to(ratio, (128, 128))
        if i < 3:
            ratio = jnp.transpose(ratio)
        state, stepped = update(mean[i] * ratio, mast[i], memo[i])
        sta[i] = state
        stp[i] = stepped
        g[i, r, 0:128] = stepped.astype(BF16)

        @pl.loop(1, 8)
        def _(k):
            ag_copy(i, k).start()

        relay_copy(i, chip).start()

    def relay(i):
        @pl.loop(1, 8)
        def _(k):
            ag_copy(i, k).wait_recv()
            relay_copy(i, from_chip(k)).start()

    add_up(0)

    def one(k, total):
        small_copy(k).wait_recv()
        return total + sm_rcv[k - 1]

    total = lax.fori_loop(1, 8, one, sm_snd[r]) * 0.25
    rows = []
    for n in range(2):
        state, stepped = update(total[n : n + 1], sm_mast[n], sm_memo[n])
        sm_sta[n] = state
        sm_stp[n] = stepped
        rows.append(stepped)
    g[0, r, 128:144] = jnp.concatenate(rows + [jnp.zeros((14, 128), F32)], axis=0).astype(BF16)

    add_up(1)
    step(0)
    add_up(2)
    step(1)
    add_up(3)
    relay(0)
    step(2)
    relay(1)
    step(3)

    relay(2)
    relay(3)

    for i in range(4):
        @pl.loop(0, 8)
        def _(d):
            relay_copy(i, d).wait_recv()
        if i == 0:
            for n in range(2):
                rows = [g[0, b, 128:144].astype(F32)[n : n + 1] for b in range(16)]
                sm_g[n] = jnp.concatenate(rows, axis=0).astype(BF16)

    for i in range(4):
        @pl.loop(0, 8)
        def _(d):
            pair_copy(i, d).wait_send()
            relay_copy(i, d).wait_send()

        @pl.loop(1, 8)
        def _(k):
            rs_copy(i, k).wait_send()
            ag_copy(i, k).wait_send()

        @pl.loop(1, 16)
        def _(j):
            psum_copy(i, j).wait_send()

    @pl.loop(1, 8)
    def _(k):
        small_copy(k).wait_send()

    for copy in small_pair:
        copy.wait_send()


def finish(g, stp, sta, sm_g, sm_stp, sm_sta, *rest):
    outs, (sem, mix_sem) = rest[:18], rest[18:]
    pairs = [(g.at[i, :, 0:128], outs[i]) for i in range(3)]
    pairs += [(sm_g.at[n], outs[4 + n]) for n in range(2)]
    pairs += [(stp.at[i], outs[6 + i]) for i in range(4)] + [(sm_stp.at[n], outs[10 + n]) for n in range(2)]
    pairs += [(sta.at[i], outs[12 + i]) for i in range(4)] + [(sm_sta.at[n], outs[16 + n]) for n in range(2)]
    copies = [pltpu.make_async_copy(s, d, sem.at[n]) for n, (s, d) in enumerate(pairs)]
    copies += [
        pltpu.make_async_copy(g.at[3, b, 0:128], outs[3].at[:, 128 * b : 128 * b + 128], mix_sem.at[b]) for b in range(16)
    ]
    for copy in copies:
        copy.start()
    for copy in copies:
        copy.wait()


def shards(*args):
    partials, masters, memories = args[0:6], args[6:12], args[12:18]
    line = lambda a: a.reshape(1, 128)
    operands = (
        *[a.reshape(8, 2, 128, 128) for a in partials[0:3]],
        partials[3].reshape(128, 2048),
        partials[4], partials[5],
        *masters[0:4], *map(line, masters[4:6]),
        *memories[0:4], *map(line, memories[4:6]),
    )
    block = jax.ShapeDtypeStruct((128, 128), F32)
    row = jax.ShapeDtypeStruct((1, 128), F32)
    out_shape = (
        *[jax.ShapeDtypeStruct((16, 128, 128), BF16)] * 3,
        jax.ShapeDtypeStruct((128, 2048), BF16),
        *[jax.ShapeDtypeStruct((16, 128), BF16)] * 2,
        *[block] * 4, *[row] * 2,
        *[block] * 4, *[row] * 2,
    )
    vmem, dma = pltpu.VMEM, pltpu.SemaphoreType.DMA
    held_shape = [
        ((4, 16, 144, 128), BF16), ((4, 128, 128), F32), ((4, 128, 128), F32),
        ((2, 16, 128), BF16), ((2, 1, 128), F32), ((2, 1, 128), F32),
    ]
    held = pl.pallas_call(
        kernel,
        out_shape=[vmem(*a) for a in held_shape],
        in_specs=[pl.BlockSpec(memory_space=pltpu.HBM)] * 18,
        out_specs=[pl.BlockSpec(memory_space=pltpu.VMEM)] * 6,
        scratch_shapes=[
            vmem((4, 8, 128, 128), F32), vmem((4, 8, 128, 128), F32),
            vmem((4, 7, CODE_ROWS, 128), BF16), vmem((4, 7, CODE_ROWS, 128), BF16),
            vmem((4, 128, 128), F32), vmem((4, 128, 128), F32), vmem((4, 128, 128), F32),
            vmem((2, 1, 2048), F32), vmem((2, 1, 2048), F32),
            vmem((16, 2, 128), F32), vmem((7, 2, 128), F32),
            vmem((2, 1, 128), F32), vmem((2, 1, 128), F32),
            vmem((4, 2, 128), F32), vmem((4, 15, 2, 128), F32),
            dma((4, 8)), dma((4, 8)), dma((4, 8)), dma((4, 7)), dma((4, 7)), dma((4, 15)), dma((4, 15)),
            dma((4, 7)), dma((4, 7)), dma((4, 8)), dma((4, 8)),
            dma((12,)), dma((2,)), dma((2,)), dma((2,)), dma((7,)), dma((7,)),
        ],
        compiler_params=pltpu.CompilerParams(collective_id=0, has_side_effects=True, vmem_limit_bytes=62600 * 1024),
    )(*operands)
    outs = pl.pallas_call(
        finish,
        out_shape=out_shape,
        in_specs=[pl.BlockSpec(memory_space=pltpu.VMEM)] * 6,
        out_specs=(pl.BlockSpec(memory_space=pltpu.HBM),) * 18,
        scratch_shapes=[dma((17,)), dma((16,))],
        compiler_params=pltpu.CompilerParams(vmem_limit_bytes=2**20),
    )(*held)
    outs = list(outs)
    for i in range(3):
        outs[i] = outs[i].reshape(2048, 128)
    for i in (4, 5):
        outs[i] = outs[i].reshape(2048)
    for i in (10, 11, 16, 17):
        outs[i] = outs[i].reshape(128)
    return tuple(outs)


def solution(mesh):
    col, row = P("replica", "model"), P("model", "replica")
    per = P("replica")
    return jax.shard_map(
        shards,
        mesh=mesh,
        in_specs=(
            *[P("replica", None, "model")] * 3, P("replica", "model", None), P("replica", None), P("replica", None),
            col, col, col, row, per, per,
            col, col, col, row, per, per,
        ),
        out_specs=(
            *[P(None, "model")] * 3, P("model", None), P(), P(),
            col, col, col, row, per, per,
            col, col, col, row, per, per,
        ),
        check_vma=False,
    )
```

```python
import functools

import jax
import jax.numpy as jnp
from jax import lax
from jax.experimental import pallas as pl
from jax.experimental.pallas import tpu as pltpu
from jax.sharding import PartitionSpec as P

LEARN_RATE = 0.015
HOLD_RATE = 0.8
F32, BF16 = jnp.float32, jnp.bfloat16

CODE_ROWS = 136


def turned(line, to_lanes):
    shape = (128, 128)
    same = lax.broadcasted_iota(jnp.int32, shape, 0) == lax.broadcasted_iota(jnp.int32, shape, 1)
    return jnp.sum(jnp.where(same, line, 0.0), axis=0 if to_lanes else 1, keepdims=True)


def encode(x, i):
    size = jnp.abs(x)
    top = jnp.max(size, axis=0 if i == 3 else 1, keepdims=True)
    top = (top * 1.004 + 1e-30).astype(BF16).astype(F32)
    size = size * (1.0 / top)
    code = jnp.exp2(250.0 * (size * lax.rsqrt(size + 1e-35)) - 125.0)
    code = jnp.where(x < 0, -code, code).astype(BF16)
    line = top if i == 3 else turned(top, True)
    return code, jnp.broadcast_to(line, (CODE_ROWS - 128, 128)).astype(BF16)


def decode(code, line, i):
    code = code.astype(F32)
    line = line.astype(F32)[0:1]
    top = line if i == 3 else turned(line, False)
    root = jnp.log2(jnp.abs(code)) * (1.0 / 250.0) + 0.5
    size = root * root * top
    return jnp.where(code < 0, -size, size)


def update(mean, master, memory):
    state = HOLD_RATE * memory + (1.0 - HOLD_RATE) * mean * mean
    return state, master - LEARN_RATE * mean * lax.rsqrt(state + 1e-06)


def kernel(*refs):
    (pq, pk, pv, pm, pn, pb, *rest) = refs
    masters, small_masters, memories, small_memories, rest = (
        rest[0:4], rest[4:6], rest[6:10], rest[10:12], rest[12:],
    )
    (
        g, stp, sta, sm_g, sm_stp, sm_sta,
        own, pair, snd, rcv, mean, mast, memo,
        sm_own, sm_pair, sm_snd, sm_rcv, sm_mast, sm_memo,
        psnd, pmid, pxr, pzr,
        own_sem, in_sem, pair_s, first_r, pair_r, smp_s, smp_r, smr_s, smr_r,
        rs_s, rs_r, px_s, px_r, pz_s, pz_r, ag_s, ag_r, last_r, rl_s, rl_r,
    ) = rest
    r, m = lax.axis_index("replica"), lax.axis_index("model")
    c = lax.rem(r, 2)
    chip = r // 2
    z, y = chip // 4, lax.rem(chip, 4)
    partner = r + 1 - 2 * c

    def to_chip(k):
        return lax.rem(z + k // 4, 2) * 4 + lax.rem(y + lax.rem(k, 4), 4)

    def from_chip(k):
        return lax.rem(z + k // 4, 2) * 4 + lax.rem(y + 4 - lax.rem(k, 4), 4)

    def x_peer(j):
        return m // 4 * 4 + lax.rem(m + j, 4)

    def z_peer(j):
        return lax.rem(m + 4 * j, 16)

    def remote(src, dst, send, recv, replica, model=None):
        return pltpu.make_async_remote_copy(
            src_ref=src, dst_ref=dst, send_sem=send, recv_sem=recv,
            device_id={"replica": replica, "model": m if model is None else model},
            device_id_type=pl.DeviceIdType.MESH,
        )

    def wait_bytes(ref, sem):
        pltpu.make_async_copy(ref, ref, sem).wait()

    barrier = pltpu.get_barrier_semaphore()

    def hail(replica, model):
        pl.semaphore_signal(
            barrier, inc=1, device_id={"replica": replica, "model": model},
            device_id_type=pl.DeviceIdType.MESH,
        )

    for j in (2, 1, 3):
        hail(r, z_peer(j))
    for j in (2, 1, 3):
        hail(r, x_peer(j))

    @pl.loop(1, 8)
    def _(k):
        hail(2 * to_chip(k) + c, m)

    hail(partner, m)

    def cut(i, d, core):
        if i < 3:
            return (pq, pk, pv)[i].at[d, core]
        return pm.at[:, pl.ds(pl.multiple_of((2 * d + core) * 128, 128), 128)]

    for i in range(3):
        pltpu.make_async_copy((pq, pk, pv)[i].at[:, c], own.at[i], own_sem.at[i]).start()

    @pl.loop(0, 8)
    def _(d):
        pltpu.make_async_copy(cut(3, d, c), own.at[3, d], own_sem.at[3]).start()

    for i in range(4):
        pltpu.make_async_copy(masters[i], mast.at[i], in_sem.at[0]).start()
        pltpu.make_async_copy(memories[i], memo.at[i], in_sem.at[1]).start()
    for n in range(2):
        pltpu.make_async_copy((pn, pb)[n], sm_own.at[n], in_sem.at[2]).start()
        pltpu.make_async_copy(small_masters[n], sm_mast.at[n], in_sem.at[3]).start()
        pltpu.make_async_copy(small_memories[n], sm_memo.at[n], in_sem.at[4]).start()

    pl.semaphore_wait(barrier, 14)

    def first_copy(d):
        return remote(cut(0, d, 1 - c), pair.at[0, d], pair_s.at[0], first_r.at[d], partner)

    @pl.loop(1, 9)
    def _(k):
        first_copy(to_chip(lax.rem(k, 8))).start()

    for i in (1, 2):
        remote((pq, pk, pv)[i].at[:, 1 - c], pair.at[i], pair_s.at[i], pair_r.at[i - 1], partner).start()
    for n in range(2):
        remote((pn, pb)[n], sm_pair.at[n], smp_s, smp_r, partner).start()

    @pl.loop(0, 8)
    def _(d):
        remote(cut(3, d, 1 - c), pair.at[3, d], pair_s.at[3], pair_r.at[2], partner).start()

    wait_bytes(mast, in_sem.at[0])

    def sizes(x, i):
        x = x * x
        return jnp.sum(x if i == 3 else jnp.transpose(x), axis=0, keepdims=True)

    for i in range(4):
        psnd[i, 1:2, :] = sizes(mast[i], i)

    def rs_copy(i, k):
        return remote(snd.at[i, k - 1], rcv.at[i, k - 1], rs_s, rs_r.at[i], 2 * to_chip(k) + c)

    def code(i, send):
        wait_bytes(own.at[i], own_sem.at[i])
        if i > 0:
            wait_bytes(pair.at[i], pair_r.at[i - 1])

        @pl.loop(1, 8)
        def _(k):
            d = to_chip(k)
            if i == 0:
                first_copy(d).wait_recv()
            snd[i, k - 1, 0:128], snd[i, k - 1, 128:CODE_ROWS] = encode(own[i, d] + pair[i, d], i)
            if send:
                rs_copy(i, k).start()

        if i == 0:
            first_copy(chip).wait_recv()
        mean[i] = own[i, chip] + pair[i, chip]

    def send(i):
        @pl.loop(1, 8)
        def _(k):
            rs_copy(i, k).start()

    def small_copy(k):
        return remote(sm_snd.at[2 * to_chip(k) + c], sm_rcv.at[k - 1], smr_s, smr_r, 2 * to_chip(k) + c)

    def send_small():
        wait_bytes(sm_own, in_sem.at[2])
        wait_bytes(sm_pair, smp_r)
        for n in range(2):
            line = sm_own[n] + sm_pair[n]
            for b in range(16):
                sm_snd[b, n : n + 1, :] = line[:, 128 * b : 128 * b + 128]

        @pl.loop(1, 8)
        def _(k):
            small_copy(k).start()

    def add_up(i):
        wait_bytes(rcv.at[i], rs_r.at[i])

        def one(k, total):
            return total + decode(rcv[i, k, 0:128], rcv[i, k, 128:CODE_ROWS], i)

        total = lax.fori_loop(0, 7, one, mean[i]) * 0.25
        mean[i] = total
        psnd[i, 0:1, :] = sizes(total, i)
        for j in range(1, 4):
            remote(psnd.at[i], pxr.at[i, j - 1], px_s, px_r.at[i], r, x_peer(j)).start()

    def across(i):
        wait_bytes(pxr.at[i], px_r.at[i])
        pmid[i] = psnd[i] + pxr[i, 0] + pxr[i, 1] + pxr[i, 2]
        for j in range(1, 4):
            remote(pmid.at[i], pzr.at[i, j - 1], pz_s, pz_r.at[i], r, z_peer(j)).start()

    height = (144, 128, 128, 128)

    def ag_copy(i, k):
        b = g.at[i, r, 0 : height[i]]
        return remote(b, b, ag_s.at[i], last_r.at[k - 1] if i == 3 else ag_r.at[i], 2 * to_chip(k) + c)

    def relay_copy(i, d):
        b = g.at[i, 2 * d + c, 0 : height[i]]
        return remote(b, b, rl_s.at[i], rl_r.at[i], partner)

    def step(i):
        wait_bytes(pzr.at[i], pz_r.at[i])
        total = pmid[i] + pzr[i, 0] + pzr[i, 1] + pzr[i, 2]
        ratio = jnp.sqrt(total[1:2]) * lax.rsqrt(total[0:1] + 1e-06)
        ratio = jnp.broadcast_to(ratio, (128, 128))
        if i < 3:
            ratio = jnp.transpose(ratio)
        state, stepped = update(mean[i] * ratio, mast[i], memo[i])
        g[i, r, 0:128] = stepped.astype(BF16)
        sta[i] = state
        stp[i] = stepped

        @pl.loop(1, 8)
        def _(k):
            ag_copy(i, k).start()

        relay_copy(i, chip).start()

    def relay(i):
        if i < 3:
            wait_bytes(g.at[i, 0:7, 0 : height[i]], ag_r.at[i])

        @pl.loop(1, 8)
        def _(k):
            if i == 3:
                ag_copy(i, k).wait_recv()
            relay_copy(i, from_chip(k)).start()

    def step_small():
        wait_bytes(sm_rcv, smr_r)
        total = sm_snd[r]
        for k in range(7):
            total = total + sm_rcv[k]
        total = total * 0.25
        wait_bytes(sm_mast, in_sem.at[3])
        wait_bytes(sm_memo, in_sem.at[4])
        rows = []
        for n in range(2):
            state, stepped = update(total[n : n + 1], sm_mast[n], sm_memo[n])
            sm_sta[n] = state
            sm_stp[n] = stepped
            rows.append(stepped)
        g[0, r, 128:144] = jnp.concatenate(rows + [jnp.zeros((14, 128), F32)], axis=0).astype(BF16)

    code(0, True)
    code(1, True)
    send_small()
    code(2, False)
    code(3, False)
    add_up(0)
    send(2)
    step_small()
    wait_bytes(memo, in_sem.at[1])
    across(0)
    add_up(1)
    send(3)
    across(1)
    add_up(2)
    step(0)
    across(2)
    add_up(3)
    step(1)
    across(3)
    relay(0)
    step(2)
    relay(1)
    step(3)
    relay(2)
    relay(3)

    for i in range(4):
        wait_bytes(g.at[i, 0:8, 0 : height[i]], rl_r.at[i])
        if i == 0:
            for n in range(2):
                rows = [g[0, b, 128:144].astype(F32)[n : n + 1] for b in range(16)]
                sm_g[n] = jnp.concatenate(rows, axis=0).astype(BF16)

    for i in range(4):
        wait_bytes(pair.at[i], pair_s.at[i])
        wait_bytes(g.at[i, 0:7, 0 : height[i]], ag_s.at[i])
        wait_bytes(g.at[i, 0:8, 0 : height[i]], rl_s.at[i])
    wait_bytes(sm_pair, smp_s)
    wait_bytes(sm_rcv, smr_s)
    wait_bytes(snd, rs_s)
    wait_bytes(pxr, px_s)
    wait_bytes(pzr, pz_s)


def finish(g, stp, sta, sm_g, sm_stp, sm_sta, *rest):
    outs, sem = rest[:18], rest[18]
    pairs = [(g.at[i, :, 0:128], outs[i]) for i in range(3)]
    pairs += [(g.at[3, b, 0:128], outs[3].at[:, 128 * b : 128 * b + 128]) for b in range(16)]
    pairs += [(sm_g.at[n], outs[4 + n]) for n in range(2)]
    pairs += [(stp.at[i], outs[6 + i]) for i in range(4)] + [(sm_stp.at[n], outs[10 + n]) for n in range(2)]
    pairs += [(sta.at[i], outs[12 + i]) for i in range(4)] + [(sm_sta.at[n], outs[16 + n]) for n in range(2)]
    for src, dst in pairs:
        pltpu.make_async_copy(src, dst, sem).start()
    for src, dst in pairs:
        pltpu.make_async_copy(src, dst, sem).wait()


def shards(*args):
    partials, masters, memories = args[0:6], args[6:12], args[12:18]
    line = lambda a: a.reshape(1, 128)
    operands = (
        *[a.reshape(8, 2, 128, 128) for a in partials[0:3]],
        partials[3].reshape(128, 2048),
        partials[4], partials[5],
        *masters[0:4], *map(line, masters[4:6]),
        *memories[0:4], *map(line, memories[4:6]),
    )
    block = jax.ShapeDtypeStruct((128, 128), F32)
    row = jax.ShapeDtypeStruct((1, 128), F32)
    out_shape = (
        *[jax.ShapeDtypeStruct((16, 128, 128), BF16)] * 3,
        jax.ShapeDtypeStruct((128, 2048), BF16),
        *[jax.ShapeDtypeStruct((16, 128), BF16)] * 2,
        *[block] * 4, *[row] * 2,
        *[block] * 4, *[row] * 2,
    )
    vmem, dma = pltpu.VMEM, pltpu.SemaphoreType.DMA
    held_shape = [
        ((4, 16, 144, 128), BF16), ((4, 128, 128), F32), ((4, 128, 128), F32),
        ((2, 16, 128), BF16), ((2, 1, 128), F32), ((2, 1, 128), F32),
    ]
    held = pl.pallas_call(
        kernel,
        out_shape=[vmem(*a) for a in held_shape],
        in_specs=[pl.BlockSpec(memory_space=pltpu.HBM)] * 18,
        out_specs=[pl.BlockSpec(memory_space=pltpu.VMEM)] * 6,
        scratch_shapes=[
            vmem((4, 8, 128, 128), F32), vmem((4, 8, 128, 128), F32),
            vmem((4, 7, CODE_ROWS, 128), BF16), vmem((4, 7, CODE_ROWS, 128), BF16),
            vmem((4, 128, 128), F32), vmem((4, 128, 128), F32), vmem((4, 128, 128), F32),
            vmem((2, 1, 2048), F32), vmem((2, 1, 2048), F32),
            vmem((16, 2, 128), F32), vmem((7, 2, 128), F32),
            vmem((2, 1, 128), F32), vmem((2, 1, 128), F32),
            vmem((4, 2, 128), F32), vmem((4, 2, 128), F32), vmem((4, 3, 2, 128), F32), vmem((4, 3, 2, 128), F32),
            dma((4,)), dma((5,)), dma((4,)), dma((8,)), dma((3,)), dma, dma, dma, dma,
            dma, dma((4,)), dma, dma((4,)), dma, dma((4,)), dma((4,)), dma((3,)), dma((7,)), dma((4,)), dma((4,)),
        ],
        compiler_params=pltpu.CompilerParams(collective_id=0, has_side_effects=True, vmem_limit_bytes=62600 * 1024),
    )(*operands)
    outs = pl.pallas_call(
        finish,
        out_shape=out_shape,
        in_specs=[pl.BlockSpec(memory_space=pltpu.VMEM)] * 6,
        out_specs=(pl.BlockSpec(memory_space=pltpu.HBM),) * 18,
        scratch_shapes=[dma],
        compiler_params=pltpu.CompilerParams(vmem_limit_bytes=2**20),
    )(*held)
    outs = list(outs)
    for i in range(3):
        outs[i] = outs[i].reshape(2048, 128)
    for i in (4, 5):
        outs[i] = outs[i].reshape(2048)
    for i in (10, 11, 16, 17):
        outs[i] = outs[i].reshape(128)
    return tuple(outs)


def solution(mesh):
    col, row = P("replica", "model"), P("model", "replica")
    per = P("replica")
    return jax.shard_map(
        shards,
        mesh=mesh,
        in_specs=(
            *[P("replica", None, "model")] * 3, P("replica", "model", None), P("replica", None), P("replica", None),
            col, col, col, row, per, per,
            col, col, col, row, per, per,
        ),
        out_specs=(
            *[P(None, "model")] * 3, P("model", None), P(), P(),
            col, col, col, row, per, per,
            col, col, col, row, per, per,
        ),
        check_vma=False,
    )
```

```python
import functools

import jax
import jax.numpy as jnp
from jax import lax
from jax.experimental import pallas as pl
from jax.experimental.pallas import tpu as pltpu
from jax.sharding import PartitionSpec as P

LEARN_RATE = 0.015
HOLD_RATE = 0.8
F32, BF16 = jnp.float32, jnp.bfloat16

CODE_ROWS = 136

SUMS = ("direct", "direct", "direct", "direct")
GATHERS = ("y first", "z first", "y first", "direct")


def turned(line, to_lanes):
    shape = (128, 128)
    same = lax.broadcasted_iota(jnp.int32, shape, 0) == lax.broadcasted_iota(jnp.int32, shape, 1)
    return jnp.sum(jnp.where(same, line, 0.0), axis=0 if to_lanes else 1, keepdims=True)


def encode(x, i):
    size = jnp.abs(x)
    top = jnp.max(size, axis=0 if i == 3 else 1, keepdims=True)
    top = (top * 1.004 + 1e-30).astype(BF16).astype(F32)
    size = size * (1.0 / top)
    code = jnp.exp2(250.0 * (size * lax.rsqrt(size + 1e-35)) - 125.0)
    code = jnp.where(x < 0, -code, code).astype(BF16)
    line = top if i == 3 else turned(top, True)
    return code, jnp.broadcast_to(line, (CODE_ROWS - 128, 128)).astype(BF16)


def decode(code, top):
    code = code.astype(F32)
    root = jnp.log2(jnp.abs(code)) * (1.0 / 250.0) + 0.5
    size = root * root * top
    return jnp.where(code < 0, -size, size)


def update(mean, master, memory):
    state = HOLD_RATE * memory + (1.0 - HOLD_RATE) * mean * mean
    return state, master - LEARN_RATE * mean * lax.rsqrt(state + 1e-06)


def kernel(*refs):
    (pq, pk, pv, pm, pn, pb, *rest) = refs
    masters, small_masters, memories, small_memories, rest = (
        rest[0:4], rest[4:6], rest[6:10], rest[10:12], rest[12:],
    )
    (
        g, stp, sta, sm_g, sm_stp, sm_sta,
        both, pair, snd, rcv, mean, mast, memo,
        sm_own, sm_pair, sm_snd, sm_rcv, sm_mast, sm_memo,
        psnd, prcv,
        own_sem, in_sem, pair_s, first_r, pair_r, smp_s, smp_r, smr_s, smr_r,
        rs_s, rs_r, fold_r, ps_s, ps_r, near, ag_s, ag_r, rl_s, rl_r,
    ) = rest
    r, m = lax.axis_index("replica"), lax.axis_index("model")
    c = lax.rem(r, 2)
    chip = r // 2
    z, y = chip // 4, lax.rem(chip, 4)
    partner = r + 1 - 2 * c

    def to_chip(k):
        return lax.rem(z + k // 4, 2) * 4 + lax.rem(y + lax.rem(k, 4), 4)

    def from_chip(k):
        return lax.rem(z + k // 4, 2) * 4 + lax.rem(y + 4 - lax.rem(k, 4), 4)

    def x_peer(j):
        return m // 4 * 4 + lax.rem(m + j, 4)

    def z_peer(j):
        return lax.rem(m + 4 * j, 16)

    def remote(src, dst, send, recv, replica, model=None):
        return pltpu.make_async_remote_copy(
            src_ref=src, dst_ref=dst, send_sem=send, recv_sem=recv,
            device_id={"replica": replica, "model": m if model is None else model},
            device_id_type=pl.DeviceIdType.MESH,
        )

    def wait_bytes(ref, sem):
        pltpu.make_async_copy(ref, ref, sem).wait()

    barrier = pltpu.get_barrier_semaphore()

    def hail(replica, model):
        pl.semaphore_signal(
            barrier, inc=1, device_id={"replica": replica, "model": model},
            device_id_type=pl.DeviceIdType.MESH,
        )

    for j in (1, 3):
        hail(r, z_peer(j))
    for j in (1, 3):
        hail(r, x_peer(j))

    @pl.loop(1, 8)
    def _(k):
        hail(2 * to_chip(k) + c, m)

    hail(partner, m)

    for i in range(3):
        pltpu.make_async_copy((pq, pk, pv)[i], both.at[i], own_sem.at[i]).start()

    @pl.loop(0, 16)
    def _(b):
        cut = pm.at[:, pl.ds(pl.multiple_of(b * 128, 128), 128)]
        pltpu.make_async_copy(cut, both.at[3, b // 2, lax.rem(b, 2)], own_sem.at[3]).start()

    for i in range(4):
        pltpu.make_async_copy(masters[i], mast.at[i], in_sem.at[0]).start()
        pltpu.make_async_copy(memories[i], memo.at[i], in_sem.at[1]).start()
    for n in range(2):
        pltpu.make_async_copy((pn, pb)[n], sm_own.at[n], in_sem.at[2]).start()
        pltpu.make_async_copy(small_masters[n], sm_mast.at[n], in_sem.at[3]).start()
        pltpu.make_async_copy(small_memories[n], sm_memo.at[n], in_sem.at[4]).start()

    def sizes(x, i):
        x = x * x
        return jnp.sum(x if i == 3 else jnp.transpose(x), axis=0, keepdims=True)

    wait_bytes(both.at[0], own_sem.at[0])
    pl.semaphore_wait(barrier, 12)

    def tell(peer, n):
        for j in (1, 3):
            pl.semaphore_signal(
                near.at[n], inc=1, device_id={"replica": r, "model": peer(j)}, device_id_type=pl.DeviceIdType.MESH
            )

    tell(z_peer, 0)

    def first_copy(d):
        return remote(both.at[0, d, 1 - c], pair.at[0, d], pair_s.at[0], first_r.at[d], partner)

    @pl.loop(1, 9)
    def _(n):
        first_copy(to_chip(8 - n)).start()

    wait_bytes(sm_own, in_sem.at[2])
    for n in range(2):
        remote(sm_own.at[n], sm_pair.at[n], smp_s, smp_r, partner).start()
    for i in range(1, 4):
        wait_bytes(both.at[i], own_sem.at[i])
        remote(both.at[i, :, 1 - c], pair.at[i], pair_s.at[i], pair_r.at[i - 1], partner).start()

    def prepare():
        pl.semaphore_wait(near.at[1], 2)
        tell(x_peer, 2)
        wait_bytes(mast, in_sem.at[0])
        for i in range(4):
            psnd[i, 1:2, :] = sizes(mast[i], i)
        wait_bytes(memo, in_sem.at[1])
        wait_bytes(sm_mast, in_sem.at[3])
        wait_bytes(sm_memo, in_sem.at[4])

    def terms(i, d):
        return both[i, d, c] + pair[i, d]

    def rs_copy(i, k):
        late = isinstance(k, int) and SUMS[i] != "direct"
        if SUMS[i] == "direct":
            at = to_chip(k)
        elif SUMS[i] == "z first":
            at = to_chip(4) if not isinstance(k, int) else to_chip(k)
        else:
            at = to_chip(lax.rem(k, 4)) if not isinstance(k, int) else to_chip(k)
        return remote(snd.at[i, k - 1], rcv.at[i, k - 1], rs_s, (fold_r if late else rs_r).at[i], 2 * at + c)

    def code_block(i, k, x):
        snd[i, k - 1, 0:128], snd[i, k - 1, 128:CODE_ROWS] = encode(x, i)

    def early(i):
        return {"direct": ((1, 8),), "z first": ((4, 8),), "y first": ((5, 8), (1, 4))}[SUMS[i]]

    def code(i, send):
        if i > 0:
            wait_bytes(pair.at[i], pair_r.at[i - 1])

        for lo, hi in early(i):
            @pl.loop(0, hi - lo)
            def _(n):
                k = hi - 1 - n
                d = to_chip(k)
                if i == 0:
                    first_copy(d).wait_recv()
                code_block(i, k, terms(i, d))
                if send:
                    rs_copy(i, k).start()

        if i == 0:
            first_copy(chip).wait_recv()
        mean[i] = terms(i, chip)

    def send(i):
        for lo, hi in early(i):
            @pl.loop(0, hi - lo)
            def _(n):
                rs_copy(i, hi - 1 - n).start()

    def heard(i, k):
        line = rcv[i, k - 1, 128:CODE_ROWS].astype(F32)[0:1]
        return decode(rcv[i, k - 1, 0:128], line if i == 3 else turned(line, False))

    def fold(i):
        if SUMS[i] == "z first":
            wait_bytes(rcv.at[i, 0:4], rs_r.at[i])
            for k in (2, 1, 3):
                d = to_chip(k)
                code_block(i, k, terms(i, d) + heard(i, 4 + k))
                rs_copy(i, k).start()
        else:
            wait_bytes(rcv.at[i, 0:6], rs_r.at[i])
            d = to_chip(4)
            code_block(i, 4, terms(i, d) + heard(i, 5) + heard(i, 6) + heard(i, 7))
            rs_copy(i, 4).start()

    def small_copy(k):
        return remote(sm_snd.at[2 * to_chip(k) + c], sm_rcv.at[k - 1], smr_s, smr_r, 2 * to_chip(k) + c)

    def send_small():
        wait_bytes(sm_pair, smp_r)
        for n in range(2):
            line = sm_own[n] + sm_pair[n]
            for b in range(16):
                sm_snd[b, n : n + 1, :] = line[:, 128 * b : 128 * b + 128]

        @pl.loop(1, 8)
        def _(k):
            small_copy(k).start()

    def add_up(i):
        if SUMS[i] == "direct":
            wait_bytes(rcv.at[i], rs_r.at[i])
        else:
            last = 3 if SUMS[i] == "z first" else 1
            wait_bytes(rcv.at[i, 0:last], fold_r.at[i])

        n = 7 if SUMS[i] == "direct" else 4
        lines = [rcv[i, k, 128:CODE_ROWS].astype(F32)[0:1] for k in range(n)]
        if i < 3:
            whole = jnp.transpose(jnp.concatenate(lines + [jnp.zeros((128 - n, 128), F32)], axis=0))
            lines = [whole[:, k : k + 1] for k in range(n)]
        total = mean[i]
        for k in range(n):
            total = total + decode(rcv[i, k, 0:128], lines[k])
        total = total * 0.25
        mean[i] = total
        psnd[i, 0:1, :] = sizes(total, i)
        if i == 0:
            pl.semaphore_wait(near.at[2], 2)

        @pl.loop(1, 16)
        def _(j):
            remote(psnd.at[i], prcv.at[i, j - 1], ps_s, ps_r.at[i], r, lax.rem(m + j, 16)).start()

    height = (144, 128, 128, 128)

    def ag_copy(i, d, k, group):
        b = g.at[i, 2 * d + c, 0 : height[i]]
        return remote(b, b, ag_s.at[i], ag_r.at[i, group], 2 * to_chip(k) + c)

    def relay_copy(i, d):
        b = g.at[i, 2 * d + c, 0 : height[i]]
        return remote(b, b, rl_s.at[i], rl_r.at[i], partner)

    def step(i):
        wait_bytes(prcv.at[i], ps_r.at[i])
        total = psnd[i]
        for j in range(15):
            total = total + prcv[i, j]
        ratio = jnp.sqrt(total[1:2]) * lax.rsqrt(total[0:1] + 1e-06)
        ratio = jnp.broadcast_to(ratio, (128, 128))
        if i < 3:
            ratio = jnp.transpose(ratio)
        state, stepped = update(mean[i] * ratio, mast[i], memo[i])
        g[i, r, 0:128] = stepped.astype(BF16)
        sta[i] = state
        stp[i] = stepped

        for group, (lo, hi) in ((2, (5, 8)), (1, (4, 5)), (0, (1, 4))):
            if group == 2 and GATHERS[i] != "direct":
                continue

            @pl.loop(lo, hi)
            def _(k):
                ag_copy(i, chip, k, group).start()

        relay_copy(i, chip).start()

    def arrive(i, group):
        n = (3, 1, 3)[group]
        wait_bytes(g.at[i, 0:n, 0 : height[i]], ag_r.at[i, group])

    def pass_on(i, group):
        lo, hi = ((1, 4), (4, 5), (5, 8))[group]

        @pl.loop(lo, hi)
        def _(k):
            relay_copy(i, from_chip(k)).start()

    def forward(i):
        if GATHERS[i] == "z first":
            arrive(i, 1)

            @pl.loop(1, 4)
            def _(k):
                ag_copy(i, from_chip(4), k, 2).start()

            pass_on(i, 1)
        if GATHERS[i] == "y first":
            arrive(i, 0)

            @pl.loop(1, 4)
            def _(k):
                ag_copy(i, from_chip(k), 4, 2).start()

            pass_on(i, 0)

    def relay(i):
        for group in (0, 1, 2):
            if group == {"z first": 1, "y first": 0, "direct": None}[GATHERS[i]]:
                continue
            arrive(i, group)
            pass_on(i, group)

    def step_small():
        wait_bytes(sm_rcv, smr_r)
        total = sm_snd[r]
        for k in range(7):
            total = total + sm_rcv[k]
        total = total * 0.25
        rows = []
        for n in range(2):
            state, stepped = update(total[n : n + 1], sm_mast[n], sm_memo[n])
            sm_sta[n] = state
            sm_stp[n] = stepped
            rows.append(stepped)
        g[0, r, 128:144] = jnp.concatenate(rows + [jnp.zeros((14, 128), F32)], axis=0).astype(BF16)

    code(0, True)
    pl.semaphore_wait(near.at[0], 2)
    tell(x_peer, 1)
    send_small()
    code(1, True)
    prepare()
    code(2, True)
    code(3, False)
    add_up(0)
    send(3)
    step_small()
    add_up(1)
    add_up(2)
    add_up(3)
    step(0)
    step(1)
    step(2)
    forward(0)
    forward(1)
    step(3)
    forward(2)
    relay(0)
    relay(1)
    relay(2)
    relay(3)

    for i in range(4):
        wait_bytes(g.at[i, 0:8, 0 : height[i]], rl_r.at[i])
        if i == 0:
            for n in range(2):
                rows = [g[0, b, 128:144].astype(F32)[n : n + 1] for b in range(16)]
                sm_g[n] = jnp.concatenate(rows, axis=0).astype(BF16)

    for i in range(4):
        wait_bytes(pair.at[i], pair_s.at[i])
        wait_bytes(g.at[i, 0:7, 0 : height[i]], ag_s.at[i])
        wait_bytes(g.at[i, 0:8, 0 : height[i]], rl_s.at[i])
    wait_bytes(sm_pair, smp_s)
    wait_bytes(sm_rcv, smr_s)
    wait_bytes(snd, rs_s)
    wait_bytes(prcv, ps_s)


def finish(g, stp, sta, sm_g, sm_stp, sm_sta, *rest):
    outs, sem = rest[:18], rest[18]
    pairs = [(g.at[i, :, 0:128], outs[i]) for i in range(3)]
    pairs += [(g.at[3, b, 0:128], outs[3].at[:, 128 * b : 128 * b + 128]) for b in range(16)]
    pairs += [(sm_g.at[n], outs[4 + n]) for n in range(2)]
    pairs += [(stp.at[i], outs[6 + i]) for i in range(4)] + [(sm_stp.at[n], outs[10 + n]) for n in range(2)]
    pairs += [(sta.at[i], outs[12 + i]) for i in range(4)] + [(sm_sta.at[n], outs[16 + n]) for n in range(2)]
    for src, dst in pairs:
        pltpu.make_async_copy(src, dst, sem).start()
    for src, dst in pairs:
        pltpu.make_async_copy(src, dst, sem).wait()


def shards(*args):
    partials, masters, memories = args[0:6], args[6:12], args[12:18]
    line = lambda a: a.reshape(1, 128)
    operands = (
        *[a.reshape(8, 2, 128, 128) for a in partials[0:3]],
        partials[3].reshape(128, 2048),
        partials[4], partials[5],
        *masters[0:4], *map(line, masters[4:6]),
        *memories[0:4], *map(line, memories[4:6]),
    )
    block = jax.ShapeDtypeStruct((128, 128), F32)
    row = jax.ShapeDtypeStruct((1, 128), F32)
    out_shape = (
        *[jax.ShapeDtypeStruct((16, 128, 128), BF16)] * 3,
        jax.ShapeDtypeStruct((128, 2048), BF16),
        *[jax.ShapeDtypeStruct((16, 128), BF16)] * 2,
        *[block] * 4, *[row] * 2,
        *[block] * 4, *[row] * 2,
    )
    vmem, dma = pltpu.VMEM, pltpu.SemaphoreType.DMA
    held_shape = [
        ((4, 16, 144, 128), BF16), ((4, 128, 128), F32), ((4, 128, 128), F32),
        ((2, 16, 128), BF16), ((2, 1, 128), F32), ((2, 1, 128), F32),
    ]
    held = pl.pallas_call(
        kernel,
        out_shape=[vmem(*a) for a in held_shape],
        in_specs=[pl.BlockSpec(memory_space=pltpu.HBM)] * 18,
        out_specs=[pl.BlockSpec(memory_space=pltpu.VMEM)] * 6,
        scratch_shapes=[
            vmem((4, 8, 2, 128, 128), F32), vmem((4, 8, 128, 128), F32),
            vmem((4, 7, CODE_ROWS, 128), BF16), vmem((4, 7, CODE_ROWS, 128), BF16),
            vmem((4, 128, 128), F32), vmem((4, 128, 128), F32), vmem((4, 128, 128), F32),
            vmem((2, 1, 2048), F32), vmem((2, 1, 2048), F32),
            vmem((16, 2, 128), F32), vmem((7, 2, 128), F32),
            vmem((2, 1, 128), F32), vmem((2, 1, 128), F32),
            vmem((4, 2, 128), F32), vmem((4, 15, 2, 128), F32),
            dma((4,)), dma((5,)), dma((4,)), dma((8,)), dma((3,)), dma, dma, dma, dma,
            dma, dma((4,)), dma((4,)), dma, dma((4,)), pltpu.SemaphoreType.REGULAR((3,)),
            dma((4,)), dma((4, 3)), dma((4,)), dma((4,)),
        ],
        compiler_params=pltpu.CompilerParams(collective_id=0, has_side_effects=True, vmem_limit_bytes=62600 * 1024),
    )(*operands)
    outs = pl.pallas_call(
        finish,
        out_shape=out_shape,
        in_specs=[pl.BlockSpec(memory_space=pltpu.VMEM)] * 6,
        out_specs=(pl.BlockSpec(memory_space=pltpu.HBM),) * 18,
        scratch_shapes=[dma],
        compiler_params=pltpu.CompilerParams(vmem_limit_bytes=2**20),
    )(*held)
    outs = list(outs)
    for i in range(3):
        outs[i] = outs[i].reshape(2048, 128)
    for i in (4, 5):
        outs[i] = outs[i].reshape(2048)
    for i in (10, 11, 16, 17):
        outs[i] = outs[i].reshape(128)
    return tuple(outs)


def solution(mesh):
    col, row = P("replica", "model"), P("model", "replica")
    per = P("replica")
    return jax.shard_map(
        shards,
        mesh=mesh,
        in_specs=(
            *[P("replica", None, "model")] * 3, P("replica", "model", None), P("replica", None), P("replica", None),
            col, col, col, row, per, per,
            col, col, col, row, per, per,
        ),
        out_specs=(
            *[P(None, "model")] * 3, P("model", None), P(), P(),
            col, col, col, row, per, per,
            col, col, col, row, per, per,
        ),
        check_vma=False,
    )
```

```python
import functools

import jax
import jax.numpy as jnp
from jax import lax
from jax.experimental import pallas as pl
from jax.experimental.pallas import tpu as pltpu
from jax.sharding import PartitionSpec as P

LEARN_RATE = 0.015
HOLD_RATE = 0.8
F32, BF16 = jnp.float32, jnp.bfloat16

PIECES = ((3, 0, 128), (0, 0, 64), (0, 64, 128), (1, 0, 64), (1, 64, 128), (2, 0, 64), (2, 64, 128))
WITH_SMALL = 2
GATHERS = ("direct", "y first", "z first", "direct", "direct", "direct", "direct")


def encode(x, i):
    rows = x.shape[0]
    size = jnp.abs(x)
    top = jnp.max(size, axis=0 if i == 3 else 1, keepdims=True)
    top = (top * 1.004 + 1e-30).astype(BF16).astype(F32)
    size = size * (1.0 / top)
    code = jnp.exp2(250.0 * (size * lax.rsqrt(size + 1e-35)) - 125.0)
    code = jnp.where(x < 0, -code, code).astype(BF16)
    if i < 3:
        shape = (rows, 128)
        same = lax.broadcasted_iota(jnp.int32, shape, 0) == lax.broadcasted_iota(jnp.int32, shape, 1)
        top = jnp.sum(jnp.where(same, top, 0.0), axis=0, keepdims=True)
    return code, jnp.broadcast_to(top, (8, 128)).astype(BF16)


def decode(code, top):
    code = code.astype(F32)
    root = jnp.log2(jnp.abs(code)) * (1.0 / 250.0) + 0.5
    size = root * root * top
    return jnp.where(code < 0, -size, size)


def update(mean, master, memory):
    state = HOLD_RATE * memory + (1.0 - HOLD_RATE) * mean * mean
    return state, master - LEARN_RATE * mean * lax.rsqrt(state + 1e-06)


def kernel(*refs):
    (pq, pk, pv, pm, pn, pb, *rest) = refs
    masters, small_masters, memories, small_memories, rest = (
        rest[0:4], rest[4:6], rest[6:10], rest[10:12], rest[12:],
    )
    (
        g, stp, sta, sm_g, sm_stp, sm_sta,
        both, pair, snd, rcv, mean, mast, memo,
        sm_own, sm_pair, sm_snd, sm_rcv, sm_mast, sm_memo,
        psnd, prcv,
        own_sem, in_sem, pair_s, first_r, pair_r, smp_s, smp_r, smr_s, smr_r,
        rs_s, rs_r, ps_s, ps_r, near, ag_s, ag_r, rl_s, rl_r,
    ) = rest
    r, m = lax.axis_index("replica"), lax.axis_index("model")
    c = lax.rem(r, 2)
    chip = r // 2
    z, y = chip // 4, lax.rem(chip, 4)
    partner = r + 1 - 2 * c

    def to_chip(k):
        return lax.rem(z + k // 4, 2) * 4 + lax.rem(y + lax.rem(k, 4), 4)

    def from_chip(k):
        return lax.rem(z + k // 4, 2) * 4 + lax.rem(y + 4 - lax.rem(k, 4), 4)

    def x_peer(j):
        return m // 4 * 4 + lax.rem(m + j, 4)

    def z_peer(j):
        return lax.rem(m + 4 * j, 16)

    def remote(src, dst, send, recv, replica, model=None):
        return pltpu.make_async_remote_copy(
            src_ref=src, dst_ref=dst, send_sem=send, recv_sem=recv,
            device_id={"replica": replica, "model": m if model is None else model},
            device_id_type=pl.DeviceIdType.MESH,
        )

    def wait_bytes(ref, sem):
        pltpu.make_async_copy(ref, ref, sem).wait()

    barrier = pltpu.get_barrier_semaphore()

    def hail(replica, model):
        pl.semaphore_signal(
            barrier, inc=1, device_id={"replica": replica, "model": model},
            device_id_type=pl.DeviceIdType.MESH,
        )

    for j in (1, 3):
        hail(r, z_peer(j))
    for j in (1, 3):
        hail(r, x_peer(j))

    @pl.loop(1, 8)
    def _(k):
        hail(2 * to_chip(k) + c, m)

    hail(partner, m)

    @pl.loop(0, 16)
    def _(b):
        cut = pm.at[:, pl.ds(pl.multiple_of(b * 128, 128), 128)]
        pltpu.make_async_copy(cut, both.at[3, b // 2, lax.rem(b, 2)], own_sem.at[3]).start()

    for i in range(3):
        pltpu.make_async_copy((pq, pk, pv)[i], both.at[i], own_sem.at[i]).start()
    for i in range(4):
        pltpu.make_async_copy(masters[i], mast.at[i], in_sem.at[0]).start()
        pltpu.make_async_copy(memories[i], memo.at[i], in_sem.at[1]).start()
    for n in range(2):
        pltpu.make_async_copy((pn, pb)[n], sm_own.at[n], in_sem.at[2]).start()
        pltpu.make_async_copy(small_masters[n], sm_mast.at[n], in_sem.at[3]).start()
        pltpu.make_async_copy(small_memories[n], sm_memo.at[n], in_sem.at[4]).start()

    def sizes(x, i):
        x = x * x
        return jnp.sum(x if i == 3 else jnp.transpose(x), axis=0, keepdims=True)

    wait_bytes(both.at[3], own_sem.at[3])
    pl.semaphore_wait(barrier, 12)

    def tell(peer, n):
        for j in (1, 3):
            pl.semaphore_signal(
                near.at[n], inc=1, device_id={"replica": r, "model": peer(j)}, device_id_type=pl.DeviceIdType.MESH
            )

    tell(z_peer, 0)

    def first_copy(d):
        return remote(both.at[3, d, 1 - c], pair.at[3, d], pair_s.at[3], first_r.at[d], partner)

    @pl.loop(1, 9)
    def _(n):
        first_copy(to_chip(8 - n)).start()

    wait_bytes(sm_own, in_sem.at[2])
    for n in range(2):
        remote(sm_own.at[n], sm_pair.at[n], smp_s, smp_r, partner).start()
    for i in range(3):
        wait_bytes(both.at[i], own_sem.at[i])
        remote(both.at[i, :, 1 - c], pair.at[i], pair_s.at[i], pair_r.at[i], partner).start()

    def prepare():
        pl.semaphore_wait(near.at[1], 2)
        tell(x_peer, 2)
        wait_bytes(mast, in_sem.at[0])
        psnd[...] = jnp.zeros_like(psnd)
        for p, (i, lo, hi) in enumerate(PIECES):
            psnd[p, 1:2, 0 : hi - lo] = sizes(mast[i, lo:hi], i)
        wait_bytes(memo, in_sem.at[1])
        wait_bytes(sm_mast, in_sem.at[3])
        wait_bytes(sm_memo, in_sem.at[4])

    def terms(p, d):
        i, lo, hi = PIECES[p]
        return both[i, d, c, lo:hi] + pair[i, d, lo:hi]

    def rs_copy(p, k):
        rows = PIECES[p][2] - PIECES[p][1] + 8
        src, dst = snd.at[p, k - 1, 0:rows], rcv.at[p, k - 1, 0:rows]
        return remote(src, dst, rs_s.at[p], rs_r.at[p], 2 * to_chip(k) + c)

    def code(p, send):
        i, lo, hi = PIECES[p]
        if p > 0 and lo == 0:
            wait_bytes(pair.at[i], pair_r.at[i])

        rows = hi - lo
        for group in ((7, 6), (5, 4), (3, 2), (1,)) if p == 0 else ((7, 6, 5, 4), (3, 2, 1)):
            if p == 0:
                for k in group:
                    first_copy(to_chip(k)).wait_recv()
            codes = [encode(terms(p, to_chip(k)), i) for k in group]
            for k, (values, tops) in zip(group, codes):
                snd[p, k - 1, 0:rows] = values
                snd[p, k - 1, rows : rows + 8] = tops
            if send:
                for k in group:
                    rs_copy(p, k).start()

        if p == 0:
            first_copy(chip).wait_recv()
        mean[i, lo:hi] = terms(p, chip)

    def send(p):
        @pl.loop(0, 7)
        def _(n):
            rs_copy(p, 7 - n).start()

    def small_copy(k):
        return remote(sm_snd.at[2 * to_chip(k) + c], sm_rcv.at[k - 1], smr_s, smr_r, 2 * to_chip(k) + c)

    def send_small():
        wait_bytes(sm_pair, smp_r)
        for n in range(2):
            line = sm_own[n] + sm_pair[n]
            for b in range(16):
                sm_snd[b, n : n + 1, :] = line[:, 128 * b : 128 * b + 128]

        @pl.loop(1, 8)
        def _(k):
            small_copy(k).start()

    def add_up(p):
        i, lo, hi = PIECES[p]
        rows = hi - lo
        wait_bytes(rcv.at[p, :, 0 : rows + 8], rs_r.at[p])
        tops = [rcv[p, k, rows : rows + 8].astype(F32)[0:1] for k in range(7)]
        if i < 3:
            whole = jnp.transpose(jnp.concatenate(tops + [jnp.zeros((121, 128), F32)], axis=0))
            tops = [whole[0:rows, k : k + 1] for k in range(7)]
        total = mean[i, lo:hi]
        for k in range(7):
            total = total + decode(rcv[p, k, 0:rows], tops[k])
        total = total * 0.25
        mean[i, lo:hi] = total
        psnd[p, 0:1, 0:rows] = sizes(total, i)
        if p == 0:
            pl.semaphore_wait(near.at[2], 2)

        @pl.loop(1, 16)
        def _(j):
            remote(psnd.at[p], prcv.at[p, j - 1], ps_s, ps_r.at[p], r, lax.rem(m + j, 16)).start()

    def rows_of(p):
        i, lo, hi = PIECES[p]
        return i, lo, hi + (16 if p == WITH_SMALL else 0)

    def ag_copy(p, d, k, group):
        i, lo, hi = rows_of(p)
        b = g.at[i, 2 * d + c, lo:hi]
        return remote(b, b, ag_s.at[p], ag_r.at[p, group], 2 * to_chip(k) + c)

    def relay_copy(p, d):
        i, lo, hi = rows_of(p)
        b = g.at[i, 2 * d + c, lo:hi]
        return remote(b, b, rl_s.at[p], rl_r.at[p], partner)

    def wait_blocks(p, n, sem):
        i, lo, hi = rows_of(p)
        wait_bytes(g.at[i, 0:n, lo:hi], sem)

    def step(p):
        i, lo, hi = PIECES[p]
        wait_bytes(prcv.at[p], ps_r.at[p])
        total = psnd[p]
        for j in range(15):
            total = total + prcv[p, j]
        ratio = jnp.sqrt(total[1:2]) * lax.rsqrt(total[0:1] + 1e-06)
        ratio = jnp.broadcast_to(ratio, (128, 128))
        if i < 3:
            ratio = jnp.transpose(ratio)[0 : hi - lo]
        state, stepped = update(mean[i, lo:hi] * ratio, mast[i, lo:hi], memo[i, lo:hi])
        g[i, r, lo:hi] = stepped.astype(BF16)
        sta[i, lo:hi] = state
        stp[i, lo:hi] = stepped

        for group, (first, last) in ((2, (5, 8)), (1, (4, 5)), (0, (1, 4))):
            if group == 2 and GATHERS[p] != "direct":
                continue

            @pl.loop(first, last)
            def _(k):
                ag_copy(p, chip, k, group).start()

        relay_copy(p, chip).start()

    def arrive(p, group):
        wait_blocks(p, (3, 1, 3)[group], ag_r.at[p, group])

    def pass_on(p, group):
        first, last = ((1, 4), (4, 5), (5, 8))[group]

        @pl.loop(first, last)
        def _(k):
            relay_copy(p, from_chip(k)).start()

    def forward(p):
        if GATHERS[p] == "z first":
            arrive(p, 1)

            @pl.loop(1, 4)
            def _(k):
                ag_copy(p, from_chip(4), k, 2).start()

            pass_on(p, 1)
        if GATHERS[p] == "y first":
            arrive(p, 0)

            @pl.loop(1, 4)
            def _(k):
                ag_copy(p, from_chip(k), 4, 2).start()

            pass_on(p, 0)

    def relay(p):
        for group in (0, 1, 2):
            if group == {"z first": 1, "y first": 0, "direct": None}[GATHERS[p]]:
                continue
            arrive(p, group)
            pass_on(p, group)

    def step_small():
        wait_bytes(sm_rcv, smr_r)
        total = sm_snd[r]
        for k in range(7):
            total = total + sm_rcv[k]
        total = total * 0.25
        rows = []
        for n in range(2):
            state, stepped = update(total[n : n + 1], sm_mast[n], sm_memo[n])
            sm_sta[n] = state
            sm_stp[n] = stepped
            rows.append(stepped)
        g[0, r, 128:144] = jnp.concatenate(rows + [jnp.zeros((14, 128), F32)], axis=0).astype(BF16)

    code(0, True)
    pl.semaphore_wait(near.at[0], 2)
    tell(x_peer, 1)
    send_small()
    code(1, True)
    prepare()
    code(2, True)
    code(3, True)
    code(4, False)
    code(5, False)
    code(6, False)
    add_up(0)
    send(4)
    add_up(1)
    send(5)
    add_up(2)
    send(6)
    step_small()
    add_up(3)
    add_up(4)
    add_up(5)
    step(0)
    add_up(6)
    step(1)
    step(2)
    step(3)
    step(4)
    forward(1)
    forward(2)
    step(5)
    relay(0)
    step(6)
    relay(1)
    relay(2)
    relay(3)
    relay(4)
    relay(5)
    relay(6)

    for p in range(7):
        wait_blocks(p, 8, rl_r.at[p])
        if p == WITH_SMALL:
            for n in range(2):
                rows = [g[0, b, 128:144].astype(F32)[n : n + 1] for b in range(16)]
                sm_g[n] = jnp.concatenate(rows, axis=0).astype(BF16)

    for i in range(4):
        wait_bytes(pair.at[i], pair_s.at[i])
    for p, (i, lo, hi) in enumerate(PIECES):
        wait_bytes(snd.at[p, :, 0 : hi - lo + 8], rs_s.at[p])
        wait_blocks(p, 7, ag_s.at[p])
        wait_blocks(p, 8, rl_s.at[p])
    wait_bytes(sm_pair, smp_s)
    wait_bytes(sm_rcv, smr_s)
    wait_bytes(prcv, ps_s)


def finish(g, stp, sta, sm_g, sm_stp, sm_sta, *rest):
    outs, sem = rest[:18], rest[18]
    pairs = [(g.at[i, :, 0:128], outs[i]) for i in range(3)]
    pairs += [(g.at[3, b, 0:128], outs[3].at[:, 128 * b : 128 * b + 128]) for b in range(16)]
    pairs += [(sm_g.at[n], outs[4 + n]) for n in range(2)]
    pairs += [(stp.at[i], outs[6 + i]) for i in range(4)] + [(sm_stp.at[n], outs[10 + n]) for n in range(2)]
    pairs += [(sta.at[i], outs[12 + i]) for i in range(4)] + [(sm_sta.at[n], outs[16 + n]) for n in range(2)]
    for src, dst in pairs:
        pltpu.make_async_copy(src, dst, sem).start()
    for src, dst in pairs:
        pltpu.make_async_copy(src, dst, sem).wait()


def shards(*args):
    partials, masters, memories = args[0:6], args[6:12], args[12:18]
    line = lambda a: a.reshape(1, 128)
    operands = (
        *[a.reshape(8, 2, 128, 128) for a in partials[0:3]],
        partials[3].reshape(128, 2048),
        partials[4], partials[5],
        *masters[0:4], *map(line, masters[4:6]),
        *memories[0:4], *map(line, memories[4:6]),
    )
    block = jax.ShapeDtypeStruct((128, 128), F32)
    row = jax.ShapeDtypeStruct((1, 128), F32)
    out_shape = (
        *[jax.ShapeDtypeStruct((16, 128, 128), BF16)] * 3,
        jax.ShapeDtypeStruct((128, 2048), BF16),
        *[jax.ShapeDtypeStruct((16, 128), BF16)] * 2,
        *[block] * 4, *[row] * 2,
        *[block] * 4, *[row] * 2,
    )
    vmem, dma = pltpu.VMEM, pltpu.SemaphoreType.DMA
    held_shape = [
        ((4, 16, 144, 128), BF16), ((4, 128, 128), F32), ((4, 128, 128), F32),
        ((2, 16, 128), BF16), ((2, 1, 128), F32), ((2, 1, 128), F32),
    ]
    held = pl.pallas_call(
        kernel,
        out_shape=[vmem(*a) for a in held_shape],
        in_specs=[pl.BlockSpec(memory_space=pltpu.HBM)] * 18,
        out_specs=[pl.BlockSpec(memory_space=pltpu.VMEM)] * 6,
        scratch_shapes=[
            vmem((4, 8, 2, 128, 128), F32), vmem((4, 8, 128, 128), F32),
            vmem((7, 7, 136, 128), BF16), vmem((7, 7, 136, 128), BF16),
            vmem((4, 128, 128), F32), vmem((4, 128, 128), F32), vmem((4, 128, 128), F32),
            vmem((2, 1, 2048), F32), vmem((2, 1, 2048), F32),
            vmem((16, 2, 128), F32), vmem((7, 2, 128), F32),
            vmem((2, 1, 128), F32), vmem((2, 1, 128), F32),
            vmem((7, 2, 128), F32), vmem((7, 15, 2, 128), F32),
            dma((4,)), dma((5,)), dma((4,)), dma((8,)), dma((3,)), dma, dma, dma, dma,
            dma((7,)), dma((7,)), dma, dma((7,)), pltpu.SemaphoreType.REGULAR((3,)),
            dma((7,)), dma((7, 3)), dma((7,)), dma((7,)),
        ],
        compiler_params=pltpu.CompilerParams(collective_id=0, has_side_effects=True, vmem_limit_bytes=62600 * 1024),
    )(*operands)
    outs = pl.pallas_call(
        finish,
        out_shape=out_shape,
        in_specs=[pl.BlockSpec(memory_space=pltpu.VMEM)] * 6,
        out_specs=(pl.BlockSpec(memory_space=pltpu.HBM),) * 18,
        scratch_shapes=[dma],
        compiler_params=pltpu.CompilerParams(vmem_limit_bytes=2**20),
    )(*held)
    outs = list(outs)
    for i in range(3):
        outs[i] = outs[i].reshape(2048, 128)
    for i in (4, 5):
        outs[i] = outs[i].reshape(2048)
    for i in (10, 11, 16, 17):
        outs[i] = outs[i].reshape(128)
    return tuple(outs)


def solution(mesh):
    col, row = P("replica", "model"), P("model", "replica")
    per = P("replica")
    return jax.shard_map(
        shards,
        mesh=mesh,
        in_specs=(
            *[P("replica", None, "model")] * 3, P("replica", "model", None), P("replica", None), P("replica", None),
            col, col, col, row, per, per,
            col, col, col, row, per, per,
        ),
        out_specs=(
            *[P(None, "model")] * 3, P("model", None), P(), P(),
            col, col, col, row, per, per,
            col, col, col, row, per, per,
        ),
        check_vma=False,
    )
```
